256 devices in a mesh: pix: 256 (over z, y, x, core).
Axes of the slice: x: 4, y: 4, z: 8, core: 2. Of those that a mesh axis runs over, the one named last changes fastest.
Arguments:
- green: float32 [16384, 6144], P('pix'), may hold values from -200 to 200, as said below
- sketch: float32 [6144, 128], P('pix'), may hold values from -0.078125 to 0.078125
Outputs:
- basis: float32 [16384, 128], P('pix')
- projection: float32 [6144, 128], P('pix')
- spectrum_gram: float32 [128, 128], replicated
The draws below stay inside these ranges and needn't reach their ends.
Inputs may be any that keep to these rules, and one draw needn't show every extreme that they name: `green`: finite real entries; each patch's column has its own scale.
All inputs are finite; a program needn't handle non-finite values.
Results may differ from the reference program's by a relative error of at most 0.000086.
Values sent between devices are 32-bit elements; how exact they have to be, the bound alone decides.
A program may use at most 64 MiB of HBM per device.

```python
import jax
import jax.numpy as jnp
from jax import lax

PATCHES = 6144
RANK = 128
PIXELS = 16384


def draw_green(key, part):
    key_cols = jax.random.fold_in(key, 11)
    key_vals = jax.random.fold_in(key, 12)
    col_scale = jnp.exp(jax.random.uniform(key_cols, (1, PATCHES), jnp.float32, jnp.log(0.3), jnp.log(3.0)))
    values = jnp.clip(jax.random.normal(key_vals, (PIXELS, PATCHES), jnp.float32), -6.0, 6.0)
    return values * col_scale


def block_scale(stream_key, shape, pieces, least, largest):
    factor_of, own = 1.0, jax.random.fold_in(stream_key, 6)
    for dim, shards_of in pieces:
        steps = jnp.exp(jax.random.uniform(jax.random.fold_in(own, dim), (shards_of,), jnp.float32, least / len(pieces), largest / len(pieces)))
        factor_of = factor_of * jnp.repeat(steps, shape[dim] // shards_of).reshape([-1 if axis == dim else 1 for axis in range(len(shape))])
    return factor_of


def noise(stream_key, shape, spread, limit, shards=(), kind=jnp.bfloat16):
    values = spread * jax.random.normal(stream_key, shape, jnp.float32)
    if shards:
        values = values * block_scale(stream_key, shape, shards, -0.22, 0.18)
    return jnp.clip(values, -limit, limit).astype(kind)


def setup_inputs(seed: int = 0) -> dict:
    arg_keys = jax.random.split(jax.random.key(seed), 3)
    return {
        "green": draw_green(jax.random.fold_in(arg_keys[2], 71), 0),
        "sketch": noise(arg_keys[1], (PATCHES, RANK), PATCHES ** -0.5, 0.078125, ((0, 256),), jnp.float32),
    }


def reference(green, sketch):
    highest = lax.Precision.HIGHEST
    sketched = jnp.dot(green.astype(jnp.float32), sketch.astype(jnp.float32), precision=highest, preferred_element_type=jnp.float32)
    gram = jnp.dot(sketched.T.astype(jnp.float32), sketched.astype(jnp.float32), precision=highest, preferred_element_type=jnp.float32)
    lower = jnp.linalg.cholesky(gram)
    orthonormal = jax.scipy.linalg.solve_triangular(lower, sketched.T, lower=True).T
    basis = jnp.sqrt(jnp.float32(PIXELS)) * orthonormal
    projection = jnp.dot(green.T.astype(jnp.float32), orthonormal.astype(jnp.float32), precision=highest, preferred_element_type=jnp.float32)
    spectrum_gram = jnp.dot(projection.T.astype(jnp.float32), projection.astype(jnp.float32), precision=highest, preferred_element_type=jnp.float32) / jnp.float32(PATCHES)
    return (basis, projection, spectrum_gram)
```

```python
import jax
import jax.numpy as jnp
from jax import lax
from jax.experimental import pallas as pl
from jax.experimental.pallas import tpu as pltpu
from jax.sharding import Mesh
from jax.sharding import PartitionSpec as P

MESH = pl.DeviceIdType.MESH
HIGHEST = lax.Precision.HIGHEST
F32 = jnp.float32
PATCHES, RANK, PIXELS = 6144, 128, 16384
NZ, NY, NX, NC = 8, 4, 4, 2
ROWS = PIXELS // (NZ * NY * NX * NC)
OWN = PATCHES // (NZ * NY * NX * NC)
PAIR = NC * OWN
HALF = PATCHES // 2
HZ = NZ // 2
PLANE = NY * NX
STRIP = 384


def dot(a, b, dims):
    return lax.dot_general(a, b, (dims, ((), ())), precision=HIGHEST, preferred_element_type=F32)


def ring(v, k, n):
    return lax.rem(v + (k % n), n)


def comm_kernel(
    green,
    sketch,
    y_out,
    b_out,
    gram_out,
    t_out,
    gg,
    om,
    ypart,
    yother,
    ychip,
    bp,
    rs1,
    rs2a,
    rs2b,
    rf1,
    rf2a,
    rf2b,
    zb,
    part,
    rsbuf,
    zbuf,
    local_sem,
    pair_send,
    pair_recv,
    agz_send,
    agz_recv,
    ag_send,
    ag_recv,
    rs_send,
    rs_recv,
    rz_send,
    rz_recv,
    ar_send,
    ar_recv,
):
    z, y, x, c = (lax.axis_index(a) for a in "zyxc")
    other = (z, y, x, 1 - c)

    def remote(src, dst, ssem, rsem, to):
        return pltpu.make_async_remote_copy(
            src_ref=src, dst_ref=dst, send_sem=ssem, recv_sem=rsem, device_id=to, device_id_type=MESH
        )

    def arrived(dst, sem):
        pltpu.make_async_copy(dst, dst, sem).wait()

    own_rows = pl.ds(pl.multiple_of(c * ROWS, ROWS), ROWS)
    mine = pltpu.make_async_copy(
        green.at[:, pl.ds(pl.multiple_of(c * HALF, HALF), HALF)], gg.at[own_rows], local_sem
    )
    mine.start()

    partners = [
        (z, ring(y, dy, NY), ring(x, dx, NX), ring(c, dc, NC))
        for dy in range(NY)
        for dx in range(NX)
        for dc in range(NC)
        if dy or dx or dc
    ] + [(ring(z, dz, NZ), y, x, ring(c, dc, NC)) for dz in range(1, NZ) for dc in range(NC)]
    barrier = pltpu.get_barrier_semaphore()
    for to in partners:
        pl.semaphore_signal(barrier, inc=1, device_id=to, device_id_type=MESH)
    pl.semaphore_wait(barrier, len(partners))

    cz = z // HZ
    zl = lax.rem(z, HZ)
    shard = om.at[zl, y, x, pl.ds(pl.multiple_of(c * OWN, OWN), OWN)]
    agz = []
    for k in range(1, NZ):
        cp = remote(sketch, shard, agz_send.at[k], agz_recv.at[zl, c], (ring(z, k, NZ), y, x, cz))
        cp.start()
        agz.append(cp)
    to_pair = remote(sketch, shard, agz_send.at[0], agz_recv.at[zl, c], other)
    to_self = pltpu.make_async_copy(sketch, shard, agz_recv.at[zl, c])

    @pl.when(cz == c)
    def _():
        to_self.start()

    @pl.when(cz != c)
    def _():
        to_pair.start()

    give = remote(
        green.at[:, pl.ds(pl.multiple_of((1 - c) * HALF, HALF), HALF)],
        gg.at[own_rows],
        pair_send.at[0],
        pair_recv.at[0],
        other,
    )
    give.start()

    sends = []

    def place(col, f, s):
        return (s, f) if col == 0 else (f, s)

    f0 = (x, y)
    s0 = (y, x)

    def f_to(col, d):
        yy, xx = place(col, ring(f0[col], d, 4), s0[col])
        return (z, yy, xx, c)

    def s_to(col, d):
        yy, xx = place(col, f0[col], ring(s0[col], d, 4))
        return (z, yy, xx, c)

    def tile(buf, col, df, ds):
        yy, xx = place(col, ring(f0[col], df, 4), ring(s0[col], ds, 4))
        return buf.at[pl.ds(2 * col, 2), yy, xx]

    def half(buf, col, h, df, ds):
        yy, xx = place(col, ring(f0[col], df, 4), ring(s0[col], ds, 4))
        return buf.at[2 * col + h, yy, xx]

    def ag(col, n, ref, to):
        cp = remote(ref, ref, ag_send.at[col, n], ag_recv.at[col, n], to)
        cp.start()
        sends.append(cp)

    for zz in range(HZ):
        for cc in range(NC):
            arrived(om.at[zz, y, x, pl.ds(cc * OWN, OWN)], agz_recv.at[zz, cc])
    QS = (0, -1, 1, 2)
    for col in range(2):
        ag(col, 0, tile(om, col, 0, 0), f_to(col, 1))
        ag(col, 1, tile(om, col, 0, 0), f_to(col, -1))
    for col in range(2):
        ag(col, 4, tile(om, col, 0, 0), s_to(col, 1))
        ag(col, 5, tile(om, col, 0, 0), s_to(col, -1))
    for col in range(2):
        arrived(tile(om, col, -1, 0), ag_recv.at[col, 0])
        ag(col, 2, half(om, col, 0, -1, 0), f_to(col, 1))
        ag(col, 6, tile(om, col, -1, 0), s_to(col, 1))
        ag(col, 7, tile(om, col, -1, 0), s_to(col, -1))
        arrived(tile(om, col, 1, 0), ag_recv.at[col, 1])
        ag(col, 3, half(om, col, 1, 1, 0), f_to(col, -1))
        ag(col, 8, tile(om, col, 1, 0), s_to(col, 1))
        ag(col, 9, tile(om, col, 1, 0), s_to(col, -1))
    for q in range(4):
        for col in range(2):
            if q == 1:
                arrived(half(om, col, 0, 2, 0), ag_recv.at[col, 2])
                arrived(half(om, col, 1, 2, 0), ag_recv.at[col, 3])
                ag(col, 10, tile(om, col, 2, 0), s_to(col, 1))
                ag(col, 11, tile(om, col, 2, 0), s_to(col, -1))
            arrived(tile(om, col, QS[q], -1), ag_recv.at[col, 4 + 2 * q])
            ag(col, 12 + 2 * q, half(om, col, 0, QS[q], -1), s_to(col, 1))
            arrived(tile(om, col, QS[q], 1), ag_recv.at[col, 5 + 2 * q])
            ag(col, 13 + 2 * q, half(om, col, 1, QS[q], 1), s_to(col, -1))
    for q in range(4):
        for col in range(2):
            arrived(half(om, col, 0, QS[q], 2), ag_recv.at[col, 12 + 2 * q])
            arrived(half(om, col, 1, QS[q], 2), ag_recv.at[col, 13 + 2 * q])

    mine.wait()
    give.wait_recv()
    acc = jnp.zeros((NC * ROWS, RANK), F32)
    per = HALF // STRIP
    ys = NY // 2
    for k in range(per):
        rows = om[k // 2, pl.ds(ys * (k % 2), ys)].reshape(STRIP, RANK)
        acc = acc + dot(gg[:, k * STRIP : (k + 1) * STRIP], rows, ((1,), (0,)))
    ypart[...] = acc
    swap = remote(ypart, yother, pair_send.at[1], pair_recv.at[1], other)
    swap.start()
    swap.wait_recv()
    ychip[...] = ypart[...] + yother[...]
    yown = ychip[own_rows, :]
    y_out[...] = yown

    me = (y * NX + x) * NC + c
    piece = pl.ds(pl.multiple_of(8 * (y * NX + x), 8), 8)

    def ar_scatter(n):
        for dy in range(NY):
            for dx in range(NX):
                for dc in range(NC):
                    if dy or dx or dc:
                        yy, xx, cc = ring(y, dy, NY), ring(x, dx, NX), ring(c, dc, NC)
                        rows = pl.ds(pl.multiple_of(8 * (yy * NX + xx), 8), 8)
                        k = (dy * NX + dx) * NC + dc
                        cp = remote(
                            part.at[n, rows],
                            rsbuf.at[n, me],
                            ar_send.at[n, k],
                            ar_recv.at[n, k],
                            (z, yy, xx, cc),
                        )
                        cp.start()
                        sends.append(cp)
        rsbuf[n, me] = part[n, piece, :]

    def ar_sum(n):
        for dy in range(NY):
            for dx in range(NX):
                for dc in range(NC):
                    if dy or dx or dc:
                        src = (ring(y, -dy, NY) * NX + ring(x, -dx, NX)) * NC + ring(c, -dc, NC)
                        k = (dy * NX + dx) * NC + dc
                        arrived(rsbuf.at[n, src], ar_recv.at[n, k])
        zbuf[n, z] = jnp.sum(rsbuf[n], axis=0)
        for dz in range(1, NZ):
            cp = remote(
                zbuf.at[n, z], zbuf.at[n, z], ar_send.at[n, 31 + dz], ar_recv.at[n, 31 + dz], (ring(z, dz, NZ), y, x, c)
            )
            cp.start()
            sends.append(cp)

    def ar_gather(n, out):
        for dz in range(1, NZ):
            arrived(zbuf.at[n, ring(z, -dz, NZ)], ar_recv.at[n, 31 + dz])
        out[piece, :] = jnp.sum(zbuf[n], axis=0)
        for dy in range(NY):
            for dx in range(NX):
                if dy or dx:
                    k = 39 + dy * NX + dx
                    cp = remote(
                        out.at[piece],
                        out.at[piece],
                        ar_send.at[n, k],
                        ar_recv.at[n, k],
                        (z, ring(y, dy, NY), ring(x, dx, NX), c),
                    )
                    cp.start()
                    sends.append(cp)

    def ar_done(n, out):
        for dy in range(NY):
            for dx in range(NX):
                if dy or dx:
                    k = 39 + dy * NX + dx
                    src = ring(y, -dy, NY) * NX + ring(x, -dx, NX)
                    rows = pl.ds(pl.multiple_of(8 * src, 8), 8)
                    arrived(out.at[rows], ar_recv.at[n, k])

    part[0] = dot(yown, yown, ((0,), (0,)))
    ar_scatter(0)

    for k in range(per):
        res = dot(gg[:, k * STRIP : (k + 1) * STRIP], ychip[...], ((0,), (0,)))
        bp[k // 2, pl.ds(ys * (k % 2), ys)] = res.reshape(ys, NX, PAIR, RANK)

    def rs(col, n, src, dst, to):
        cp = remote(src, dst, rs_send.at[col, n], rs_recv.at[col, n], to)
        cp.start()
        sends.append(cp)

    RQ = (2, -1, 1, 0)
    for q in range(4):
        for col in range(2):
            rs(col, 2 * q, half(bp, col, 0, RQ[q], 2), rs1.at[col, q, 0], s_to(col, 1))
            rs(col, 2 * q + 1, half(bp, col, 1, RQ[q], 2), rs1.at[col, q, 1], s_to(col, -1))
            rs(col, 8 + 2 * q, half(bp, col, 1, RQ[q], 1), rs2a.at[col, q, 0], s_to(col, 1))
            rs(col, 9 + 2 * q, half(bp, col, 0, RQ[q], -1), rs2a.at[col, q, 1], s_to(col, -1))

    def add(dst, *srcs):
        tot = dst[...]
        for s in srcs:
            tot = tot + s[...]
        dst[...] = tot

    def s_forward(q, col):
        arrived(rs1.at[col, q, 0], rs_recv.at[col, 2 * q])
        blk = half(bp, col, 0, RQ[q], 1)
        add(blk, rs1.at[col, q, 0])
        rs(col, 16 + 2 * q, blk, rs2b.at[col, q, 0], s_to(col, 1))
        arrived(rs1.at[col, q, 1], rs_recv.at[col, 2 * q + 1])
        blk = half(bp, col, 1, RQ[q], -1)
        add(blk, rs1.at[col, q, 1])
        rs(col, 17 + 2 * q, blk, rs2b.at[col, q, 1], s_to(col, -1))

    def s_finish(q, col):
        for d in range(2):
            arrived(rs2a.at[col, q, d], rs_recv.at[col, 8 + 2 * q + d])
            arrived(rs2b.at[col, q, d], rs_recv.at[col, 16 + 2 * q + d])
        add(half(bp, col, 0, RQ[q], 0), rs2b.at[col, q, 0], rs2a.at[col, q, 1])
        add(half(bp, col, 1, RQ[q], 0), rs2a.at[col, q, 0], rs2b.at[col, q, 1])
        if q == 0:
            rs(col, 24, half(bp, col, 0, 2, 0), rf1.at[col, 0], f_to(col, 1))
            rs(col, 25, half(bp, col, 1, 2, 0), rf1.at[col, 1], f_to(col, -1))
        if q == 1:
            rs(col, 27, half(bp, col, 0, -1, 0), rf2a.at[col, 1], f_to(col, -1))
        if q == 2:
            rs(col, 26, half(bp, col, 1, 1, 0), rf2a.at[col, 0], f_to(col, 1))
            arrived(rf1.at[col, 0], rs_recv.at[col, 24])
            blk = half(bp, col, 0, 1, 0)
            add(blk, rf1.at[col, 0])
            rs(col, 28, blk, rf2b.at[col, 0], f_to(col, 1))
            arrived(rf1.at[col, 1], rs_recv.at[col, 25])
            blk = half(bp, col, 1, -1, 0)
            add(blk, rf1.at[col, 1])
            rs(col, 29, blk, rf2b.at[col, 1], f_to(col, -1))

    for q in range(4):
        for col in range(2):
            s_forward(q, col)
        if q == 1:
            ar_sum(0)
    for q in range(4):
        for col in range(2):
            s_finish(q, col)
        if q == 1:
            ar_gather(0, gram_out)
    for col in range(2):
        for d in range(2):
            arrived(rf2a.at[col, d], rs_recv.at[col, 26 + d])
            arrived(rf2b.at[col, d], rs_recv.at[col, 28 + d])
        add(half(bp, col, 0, 0, 0), rf2b.at[col, 0], rf2a.at[col, 1])
        add(half(bp, col, 1, 0, 0), rf2a.at[col, 0], rf2b.at[col, 1])

    for zz in range(HZ):
        for cc in range(NC):
            k = zz * NC + cc
            zt = c * HZ + zz
            src = bp.at[zz, y, x, pl.ds(cc * OWN, OWN)]
            here = jnp.logical_and(zt == z, c == cc)
            far = remote(src, zb.at[z], rz_send.at[k], rz_recv.at[z], (zt, y, x, cc))
            near = pltpu.make_async_copy(src, zb.at[z], rz_recv.at[z])

            @pl.when(here)
            def _():
                near.start()

            @pl.when(jnp.logical_not(here))
            def _():
                far.start()

    ar_done(0, gram_out)
    for k in range(NZ):
        arrived(zb.at[k], rz_recv.at[k])
    b = jnp.sum(zb[...], axis=0)
    eye = lax.broadcasted_iota(jnp.int32, (RANK, RANK), 0) == lax.broadcasted_iota(jnp.int32, (RANK, RANK), 1)
    diag = jnp.sum(jnp.where(eye, gram_out[...], 0.0), axis=0, keepdims=True)
    b = b * lax.rsqrt(diag)
    b_out[...] = b
    part[1] = dot(b, b, ((0,), (0,)))
    ar_scatter(1)
    ar_sum(1)
    ar_gather(1, t_out)
    ar_done(1, t_out)

    for cp in agz:
        cp.wait_send()

    @pl.when(cz != c)
    def _():
        to_pair.wait_send()

    give.wait_send()
    swap.wait_send()
    for cp in sends:
        cp.wait_send()
    for zz in range(HZ):
        for cc in range(NC):
            k = zz * NC + cc
            zt = c * HZ + zz
            src = bp.at[zz, y, x, pl.ds(cc * OWN, OWN)]

            @pl.when(jnp.logical_not(jnp.logical_and(zt == z, c == cc)))
            def _():
                remote(src, zb.at[z], rz_send.at[k], rz_recv.at[z], (zt, y, x, cc)).wait_send()


def communicate(green, sketch):
    vm = pltpu.VMEM
    dma = pltpu.SemaphoreType.DMA
    blk = (HZ, NY, NX, PAIR, RANK)
    return pl.pallas_call(
        comm_kernel,
        name="comm",
        out_shape=[
            jax.ShapeDtypeStruct((ROWS, RANK), F32),
            jax.ShapeDtypeStruct((OWN, RANK), F32),
            jax.ShapeDtypeStruct((RANK, RANK), F32),
            jax.ShapeDtypeStruct((RANK, RANK), F32),
        ],
        in_specs=[pl.BlockSpec(memory_space=pl.ANY), pl.BlockSpec(memory_space=vm)],
        out_specs=[pl.BlockSpec(memory_space=vm)] * 4,
        scratch_shapes=[
            vm((NC * ROWS, HALF), F32),
            vm(blk, F32),
            vm((NC * ROWS, RANK), F32),
            vm((NC * ROWS, RANK), F32),
            vm((NC * ROWS, RANK), F32),
            vm(blk, F32),
            vm((2, 4, 2, PAIR, RANK), F32),
            vm((2, 4, 2, PAIR, RANK), F32),
            vm((2, 4, 2, PAIR, RANK), F32),
            vm((2, 2, PAIR, RANK), F32),
            vm((2, 2, PAIR, RANK), F32),
            vm((2, 2, PAIR, RANK), F32),
            vm((NZ, OWN, RANK), F32),
            vm((2, RANK, RANK), F32),
            vm((2, PLANE * NC, 8, RANK), F32),
            vm((2, NZ, 8, RANK), F32),
            dma,
            dma((2,)),
            dma((2,)),
            dma((NZ,)),
            dma((HZ, NC)),
            dma((2, 20)),
            dma((2, 20)),
            dma((2, 30)),
            dma((2, 30)),
            dma((NZ,)),
            dma((NZ,)),
            dma((2, 55)),
            dma((2, 55)),
        ],
        compiler_params=pltpu.CompilerParams(collective_id=0, has_side_effects=True, vmem_limit_bytes=40 * 2**20),
    )(green, sketch)


def finish_kernel(ys, bs, gram, t, basis, projection, spectrum, a, m):
    eye = lax.broadcasted_iota(jnp.int32, (RANK, RANK), 0) == lax.broadcasted_iota(jnp.int32, (RANK, RANK), 1)
    g = gram[...]
    picked = jnp.where(eye, g, 0.0)
    across = lax.rsqrt(jnp.sum(picked, axis=0, keepdims=True))
    down = lax.rsqrt(jnp.sum(picked, axis=1, keepdims=True))
    a[...] = g * across * down
    m[...] = jnp.where(eye, 1.0, 0.0)
    sub = lax.broadcasted_iota(jnp.int32, (8, RANK), 0)
    for k in range(RANK // 8):
        p = a[8 * k : 8 * k + 8, :]
        q = m[8 * k : 8 * k + 8, :]
        cols = [jnp.broadcast_to(p[:, 8 * k + j : 8 * k + j + 1], (8, RANK)) for j in range(8)]
        for j in range(8):
            pivot = jnp.broadcast_to(cols[j][j : j + 1, :], (8, RANK))
            r = lax.rsqrt(pivot)
            r = r * (1.5 - 0.5 * pivot * r * r)
            below = sub > j
            mult = jnp.where(below, cols[j] * r, 0.0)
            prow = jnp.broadcast_to(p[j : j + 1, :], (8, RANK)) * r
            qrow = jnp.broadcast_to(q[j : j + 1, :], (8, RANK)) * r
            at = sub == j
            p = jnp.where(at, prow, p - mult * prow)
            q = jnp.where(at, qrow, q - mult * qrow)
            for l in range(j + 1, 8):
                cols[l] = cols[l] - mult * (jnp.broadcast_to(cols[l][j : j + 1, :], (8, RANK)) * r)
        m[8 * k : 8 * k + 8, :] = q
        if k < RANK // 8 - 1:
            rest = slice(8 * k + 8, RANK)
            lhs = p[:, 8 * k + 8 :]
            a[rest, :] = a[rest, :] - dot(lhs, p, ((0,), (0,)))
            m[rest, :] = m[rest, :] - dot(lhs, q, ((0,), (0,)))
    inv = m[...]
    basis[...] = 128.0 * dot(ys[...] * across, inv, ((1,), (1,)))
    projection[...] = dot(bs[...], inv, ((1,), (1,)))
    spectrum[...] = dot(dot(inv, t[...], ((1,), (0,))), inv, ((1,), (1,))) / float(PATCHES)


def body(green, sketch):
    ys, bs, gram, t = communicate(green, sketch)
    vm = pltpu.VMEM
    return pl.pallas_call(
        finish_kernel,
        name="finish",
        out_shape=[
            jax.ShapeDtypeStruct((ROWS, RANK), F32),
            jax.ShapeDtypeStruct((OWN, RANK), F32),
            jax.ShapeDtypeStruct((RANK, RANK), F32),
        ],
        in_specs=[pl.BlockSpec(memory_space=vm)] * 4,
        out_specs=[pl.BlockSpec(memory_space=vm)] * 3,
        scratch_shapes=[vm((RANK, RANK), F32), vm((RANK, RANK), F32)],
    )(ys, bs, gram, t)


def solution(mesh):
    axes = ("z", "y", "x", "c")
    split = Mesh(mesh.devices.reshape(NZ, NY, NX, NC), axes)
    in_specs = (P(axes, None), P(axes, None))
    out_specs = (P(axes, None), P(axes, None), P())
    return jax.shard_map(body, mesh=split, in_specs=in_specs, out_specs=out_specs, check_vma=False)
```
